256 devices in a mesh: band: 64 (over x, z_hi, y), lev: 4 (over z_lo, core).
Axes of the slice: x: 4, y: 4, z: 8 (z_hi: 4, z_lo: 2; z = z_hi * 2 + z_lo), core: 2. Of those that a mesh axis runs over, the one named last changes fastest.
Arguments:
- pattern: float32 [8192, 128], P('band'), may hold values from -3 to 3
- taper: float32 [136], P('lev'), may hold values from 0.1 to 1
- thickness: float32 [136], P('lev'), may hold values from 0.2 to 2
- block_source: int32 [8192], P('band'), may hold values from 0 to 8191, as said below
- tendencies: bfloat16 [4, 136, 1048576], P(None, 'lev', 'band'), may hold values from -6 to 6
Outputs:
- perturbed: bfloat16 [4, 136, 1048576], P(None, 'lev', 'band')
- integrals: float32 [2, 1048576], P(None, 'band')
The draws below stay inside these ranges and needn't reach their ends.
Inputs may be any that keep to these rules, and one draw needn't show every extreme that they name: block_source is a permutation of 0 to 8191; the 128 physics blocks of each band index take exactly 128 // 64 grid blocks from the 128 grid blocks of each band index.
All inputs are finite; a program needn't handle non-finite values.
Results may differ from the reference program's by a relative error of at most 0.001.
Values sent between devices are 32-bit elements; how exact they have to be, the bound alone decides.
No kernel may reach another device: no remote copies, remote signals or barrier semaphores. Data moves between devices by JAX's collectives and lax.ppermute only.
A program may use at most 64 MiB of HBM per device.

```python
import math
import jax
import jax.numpy as jnp
from jax import lax

BLOCK = 128
LEV = 136
BLK_DEV = 128
NBLK = 8192
COLUMNS = 1048576


def draw_block_source(key, part):
    bands = NBLK // BLK_DEV
    share = BLK_DEV // bands
    first_key, second_key = jax.random.split(jax.random.fold_in(key, 11))
    labels = jnp.repeat(jnp.arange(bands, dtype=jnp.int32), share)
    owner_keys = jax.random.split(first_key, bands)
    owners = jax.vmap(lambda k: jax.random.permutation(k, labels))(owner_keys).reshape(-1)
    grouped = jnp.argsort(owners, stable=True).astype(jnp.int32).reshape(bands, BLK_DEV)
    row_keys = jax.random.split(second_key, bands)
    shuffled = jax.vmap(lambda k, row: jax.random.permutation(k, row))(row_keys, grouped)
    return shuffled.reshape(-1).astype(jnp.int32)


def steps_of(stream_key, extent, pieces, low, top_value):
    gain, own = 1.0, jax.random.fold_in(stream_key, 6)
    for position, blocks in pieces:
        draws = jnp.exp(jax.random.uniform(jax.random.fold_in(own, position), (blocks,), jnp.float32, low / len(pieces), top_value / len(pieces)))
        gain = gain * jnp.repeat(draws, extent[position] // blocks).reshape([-1 if axis == position else 1 for axis in range(len(extent))])
    return gain


def gaussian(stream_key, extent, deviation, most, shards=(), kind=jnp.bfloat16):
    result = jax.random.normal(stream_key, extent, jnp.float32) * deviation
    if len(shards) > 0:
        result = steps_of(stream_key, extent, shards, -0.22, 0.18) * result
    return jnp.clip(result, min=-most, max=most).astype(kind)


def setup_inputs(seed: int = 0) -> dict:
    keys = jax.random.split(jax.random.key(seed), 6)
    return {
        "pattern": gaussian(keys[0], (NBLK, BLOCK), 0.6, 3.0, ((0, 64),), jnp.float32),
        "taper": jnp.clip(0.1 + 0.9 * jax.random.uniform(keys[1], (LEV,), jnp.float32) ** steps_of(keys[1], (LEV,), ((0, 4),), -0.2, 0.2), 0.1, 1.0),
        "thickness": jnp.clip(jnp.exp(math.log(2.0) - 2.3025851 * jax.random.uniform(keys[2], (LEV,), jnp.float32) ** steps_of(keys[2], (LEV,), ((0, 4),), -0.2, 0.2)), 0.2, 2.0),
        "block_source": draw_block_source(jax.random.fold_in(keys[5], 71), 0),
        "tendencies": gaussian(keys[4], (4, LEV, COLUMNS), 1.0, 6.0, ((1, 4), (2, 64))),
    }


def reference(pattern, taper, thickness, block_source, tendencies):
    clipped = jnp.tanh(pattern)
    local = jnp.take(clipped, block_source, axis=0).reshape(-1)
    pert = taper[:, None] * local[None, :]

    def scale_field(field):
        return (field.astype(jnp.float32) * (1.0 + pert)).astype(jnp.bfloat16)
    perturbed = lax.map(scale_field, tendencies)

    def column_sum(field):
        return lax.optimization_barrier(jnp.sum(thickness[:, None] * field.astype(jnp.float32) * pert, axis=0))
    norm_value = jnp.sqrt(jnp.sum(thickness * thickness))
    integrals = lax.map(column_sum, tendencies[2:4]) / norm_value
    return (perturbed, integrals)
```

```python
import functools

import jax
import jax.numpy as jnp
from jax import lax
from jax.experimental import pallas as pl
from jax.experimental.pallas import tpu as pltpu
from jax.sharding import PartitionSpec as P

PLANE = [[x * 16 + z * 4 + y for x in range(4) for y in range(4)] for z in range(4)]
ROW = 128


def onto(band, step):
    return (band // 16) * 16 + ((band // 4 + step) % 4) * 4 + band % 4


def along_z(a, step):
    return lax.ppermute(a, "band", [(b, onto(b, step)) for b in range(64)])


def across_lev(a, flip):
    return lax.ppermute(a, "lev", [(i, i ^ flip) for i in range(4)])


def within_plane(a):
    return lax.all_to_all(a, "band", 0, 0, tiled=True, axis_index_groups=PLANE)


def iota(shape, dim):
    return lax.broadcasted_iota(jnp.int32, shape, dim)


def onehot(cond):
    return jnp.where(cond, 1.0, 0.0).astype(jnp.bfloat16)


def dot(a, b):
    return jnp.dot(a, b, preferred_element_type=jnp.float32)


def dot_nt(a, b):
    return lax.dot_general(a, b, (((1,), (1,)), ((), ())), preferred_element_type=jnp.float32)


def three_parts(v):
    high = v.astype(jnp.bfloat16)
    rest = v - high.astype(jnp.float32)
    mid = rest.astype(jnp.bfloat16)
    low = (rest - mid.astype(jnp.float32)).astype(jnp.bfloat16)
    return high, mid, low


def request_kernel(source_ref, ids_ref, pos_ref):
    source = source_ref[...]
    band, row = source >> 7, source & 127
    group = (band >> 4) * 4 + (band & 3)
    my_z = (lax.axis_index("band") >> 2) & 3
    table = (my_z - ((band >> 2) & 3)) & 3
    member = iota((16, ROW), 0) == group
    before = onehot(iota((ROW, ROW), 0) < iota((ROW, ROW), 1))
    count = dot(onehot(member), before)
    rank = jnp.sum(jnp.where(member, count, 0.0), axis=0, keepdims=True)
    pos = group * 8 + rank.astype(jnp.int32)
    slot = onehot(iota((ROW, ROW), 0) == pos)

    def everywhere(v):
        return jnp.broadcast_to(v.astype(jnp.float32), (ROW, ROW)).astype(jnp.bfloat16)

    ids = dot_nt(slot, everywhere(table)) * 128.0 + dot_nt(slot, everywhere(row))
    ids_ref[...] = ids.astype(jnp.int32)
    pos_ref[...] = jnp.broadcast_to(pos, pos_ref.shape)


def pick_kernel(ids_ref, t0, t1, t2, t3, out_ref):
    ids = ids_ref[...]
    lane = iota((ROW, ROW), 1)
    total = None
    for c, ref in enumerate((t0, t1, t2, t3)):
        pick = onehot(ids == lane + c * ROW)
        high, mid, low = three_parts(ref[...])
        part = (dot(pick, high), dot(pick, mid), dot(pick, low))
        total = part if total is None else tuple(a + b for a, b in zip(total, part))
    out_ref[...] = (total[0] + total[1]) + total[2]


def column_kernel(taper_ref, thick_ref, pos_ref, x_ref, sums_ref, place_ref, acc_ref):
    levels = x_ref.shape[0]
    pos = jnp.broadcast_to(pos_ref[0:1, :].astype(jnp.float32), (ROW, ROW)).astype(jnp.bfloat16)
    expand = onehot(iota((4 * ROW, ROW), 0) >> 2 == iota((4 * ROW, ROW), 1))
    slot = dot_nt(expand, pos).astype(jnp.int32)
    place_ref[...] = onehot(slot == iota((4 * ROW, ROW), 1))

    weights = [taper_ref[l] * thick_ref[l] for l in range(levels)]

    def chunk(i, carry):
        rows = pl.ds(pl.multiple_of(i * 64, 64), 64)
        acc = x_ref[0, rows, :].astype(jnp.float32) * weights[0]
        for l in range(1, levels):
            acc = acc + x_ref[l, rows, :].astype(jnp.float32) * weights[l]
        acc_ref[rows, :] = acc
        return carry

    lax.fori_loop(0, 8, chunk, 0)
    for k in range(2):
        sums_ref[pl.ds(k * ROW, ROW), :] = acc_ref[pl.ds(2 + k, ROW, stride=4), :]
    squares = thick_ref[0] * thick_ref[0]
    for l in range(1, levels):
        squares = squares + thick_ref[l] * thick_ref[l]
    sums_ref[pl.ds(2 * ROW, 8), :] = jnp.full((8, ROW), squares, jnp.float32)


def perturb_kernel(taper_ref, arrived_ref, place_ref, s0, s1, s2, s3, x_ref, y_ref, out_ref, local_ref):
    levels = x_ref.shape[0]
    step = pl.program_id(0)

    @pl.when(step == 0)
    def _():
        parts = three_parts(jnp.tanh(arrived_ref[...]))
        place = place_ref[...]
        local_ref[...] = (dot(place, parts[0]) + dot(place, parts[1])) + dot(place, parts[2])
        total = (s0[...] + s1[...]) + (s2[...] + s3[...])
        norm = jnp.sqrt(total[2 * ROW : 2 * ROW + 1, :])
        local = local_ref[pl.ds(0, ROW, stride=4), :]
        for k in range(2):
            out_ref[pl.ds(k, ROW, stride=2), :] = local * total[k * ROW : (k + 1) * ROW, :] / norm

    rows = x_ref.shape[1]
    for r in range(0, rows, 32):
        local = local_ref[pl.ds(pl.multiple_of(step * rows + r, 32), 32), :]
        for l in range(levels):
            scale = 1.0 + taper_ref[l] * local
            y_ref[l, r : r + 32, :] = (x_ref[l, r : r + 32, :].astype(jnp.float32) * scale).astype(jnp.bfloat16)


def body(pattern, taper, thickness, block_source, tendencies):
    vmem, smem = pl.BlockSpec(memory_space=pltpu.VMEM), pl.BlockSpec(memory_space=pltpu.SMEM)
    levels = tendencies.shape[1]
    f32, s32 = jnp.float32, jnp.int32

    tables = [pattern] + [along_z(pattern, k) for k in (1, 2, 3)]
    ids, pos = pl.pallas_call(
        request_kernel,
        out_shape=(jax.ShapeDtypeStruct((ROW, ROW), s32), jax.ShapeDtypeStruct((8, ROW), s32)),
        in_specs=[vmem],
        out_specs=(vmem, vmem),
        compiler_params=pltpu.CompilerParams(vmem_limit_bytes=4 << 20),
        name="request",
    )(block_source.reshape(1, ROW))
    wanted = within_plane(ids.reshape(16, 8, ROW)).reshape(ROW, ROW)

    x = tendencies.reshape(4, levels, ROW, ROW).transpose(1, 2, 0, 3).reshape(levels, 4 * ROW, ROW)
    sums, place = pl.pallas_call(
        column_kernel,
        out_shape=(jax.ShapeDtypeStruct((2 * ROW + 8, ROW), f32), jax.ShapeDtypeStruct((4 * ROW, ROW), jnp.bfloat16)),
        in_specs=[smem, smem, vmem, vmem],
        out_specs=(vmem, vmem),
        scratch_shapes=[pltpu.VMEM((4 * ROW, ROW), f32)],
        cost_estimate=pl.CostEstimate(flops=10_000_000, bytes_accessed=4_500_000, transcendentals=0),
        compiler_params=pltpu.CompilerParams(vmem_limit_bytes=12 << 20),
        name="columns",
    )(taper, thickness, pos, x)
    others = [across_lev(sums, flip) for flip in (1, 2, 3)]

    picked = pl.pallas_call(
        pick_kernel,
        out_shape=jax.ShapeDtypeStruct((ROW, ROW), f32),
        in_specs=[vmem] * 5,
        out_specs=vmem,
        compiler_params=pltpu.CompilerParams(vmem_limit_bytes=4 << 20),
        name="pick",
    )(wanted, *tables)
    arrived = within_plane(picked.reshape(16, 8, ROW)).reshape(ROW, ROW)

    steps = 8
    rows = 4 * ROW // steps
    whole = lambda shape: pl.BlockSpec(shape, lambda i: (0,) * len(shape))
    stream = pl.BlockSpec((levels, rows, ROW), lambda i: (0, i, 0))
    y, out = pl.pallas_call(
        perturb_kernel,
        grid=(steps,),
        out_shape=(jax.ShapeDtypeStruct(x.shape, x.dtype), jax.ShapeDtypeStruct((2 * ROW, ROW), f32)),
        in_specs=[smem, whole((ROW, ROW)), whole((4 * ROW, ROW))] + [whole(sums.shape)] * 4 + [stream],
        out_specs=(stream, whole((2 * ROW, ROW))),
        scratch_shapes=[pltpu.VMEM((4 * ROW, ROW), f32)],
        cost_estimate=pl.CostEstimate(flops=10_000_000, bytes_accessed=9_000_000, transcendentals=0),
        compiler_params=pltpu.CompilerParams(vmem_limit_bytes=12 << 20),
        name="perturb",
    )(taper, arrived, place, sums, *others, x)
    perturbed = y.reshape(levels, ROW, 4, ROW).transpose(2, 0, 1, 3).reshape(tendencies.shape)
    integrals = out.reshape(ROW, 2, ROW).transpose(1, 0, 2).reshape(2, ROW * ROW)
    return perturbed, integrals


def solution(mesh):
    in_specs = (P("band", None), P("lev"), P("lev"), P("band"), P(None, "lev", "band"))
    out_specs = (P(None, "lev", "band"), P(None, "band"))
    return jax.shard_map(body, mesh=mesh, in_specs=in_specs, out_specs=out_specs, check_vma=False)
```

```python
import jax
import jax.numpy as jnp
from jax import lax
from jax.experimental import pallas as pl
from jax.experimental.pallas import tpu as pltpu
from jax.sharding import PartitionSpec as P


ROW = 128
LEVELS = 40
PARTS = 8
PART = 4 * ROW // PARTS


def along_z(a, step):
    return lax.ppermute(a, "z", [(i, (i + step) % 4) for i in range(4)])


def across_lev(a, flip):
    return lax.ppermute(a, "lev", [(i, i ^ flip) for i in range(4)])


def within_plane(a):
    return lax.all_to_all(a, ("x", "y"), 0, 0, tiled=True)


def iota(shape, dim):
    return lax.broadcasted_iota(jnp.int32, shape, dim)


def onehot(cond):
    return jnp.where(cond, 1.0, 0.0).astype(jnp.bfloat16)


def dot(a, b):
    return jnp.dot(a, b, preferred_element_type=jnp.float32)


def dot_nt(a, b):
    return lax.dot_general(a, b, (((1,), (1,)), ((), ())), preferred_element_type=jnp.float32)


def three_parts(v):
    high = v.astype(jnp.bfloat16)
    rest = v - high.astype(jnp.float32)
    mid = rest.astype(jnp.bfloat16)
    low = (rest - mid.astype(jnp.float32)).astype(jnp.bfloat16)
    return high, mid, low


def request_kernel(source_ref, taper_ref, thick_ref, ids_ref, pos_ref, scalars_ref):
    source = source_ref[...]
    band, row = source >> 7, source & 127
    group = (band >> 4) * 4 + (band & 3)
    my_z = lax.axis_index("z")
    table = (my_z - ((band >> 2) & 3)) & 3
    member = iota((16, ROW), 0) == group
    before = onehot(iota((ROW, ROW), 0) < iota((ROW, ROW), 1))
    count = dot(onehot(member), before)
    rank = jnp.sum(jnp.where(member, count, 0.0), axis=0, keepdims=True)
    pos = group * 8 + rank.astype(jnp.int32)
    slot = onehot(iota((ROW, ROW), 0) == pos)

    def everywhere(v):
        return jnp.broadcast_to(v.astype(jnp.float32), (ROW, ROW)).astype(jnp.bfloat16)

    ids = dot_nt(slot, everywhere(table)) * 128.0 + dot_nt(slot, everywhere(row))
    ids_ref[...] = ids.astype(jnp.int32)
    pos_ref[...] = jnp.broadcast_to(pos, pos_ref.shape)

    taper, thick = taper_ref[...], thick_ref[...]
    levels = taper.shape[1]
    diagonal = iota((LEVELS, levels), 0) == iota((LEVELS, levels), 1)

    def one_per_row(v):
        total = jnp.sum(jnp.where(diagonal, jnp.broadcast_to(v, diagonal.shape), 0.0), axis=1, keepdims=True)
        return jnp.broadcast_to(total, (LEVELS, ROW))

    scalars_ref[0:LEVELS, :] = one_per_row(taper)
    scalars_ref[LEVELS : 2 * LEVELS, :] = one_per_row(taper * thick)
    scalars_ref[2 * LEVELS :, :] = jnp.broadcast_to(jnp.sum(thick * thick, axis=1, keepdims=True), (8, ROW))


def pick_kernel(ids_ref, t0, t1, t2, t3, out_ref):
    ids = ids_ref[...]
    lane = iota((ROW, ROW), 1)
    total = None
    for c, ref in enumerate((t0, t1, t2, t3)):
        pick = onehot(ids == lane + c * ROW)
        high, mid, low = three_parts(ref[...])
        part = (dot(pick, high), dot(pick, mid), dot(pick, low))
        total = part if total is None else tuple(a + b for a, b in zip(total, part))
    out_ref[...] = (total[0] + total[1]) + total[2]


def fetches(x_hbm, x_ref, sems):
    def fetch(i):
        rows = pl.ds(pl.multiple_of(i * PART, PART), PART)
        return pltpu.make_async_copy(x_hbm.at[:, rows, :], x_ref.at[:, rows, :], sems.at[i])

    for i in range(PARTS):
        fetch(i).start()
    return fetch


def column_kernel(scalars_ref, pos_ref, x_hbm, sums_ref, place_ref, acc_ref, x_ref, sems):
    levels = x_ref.shape[0]
    fetch = fetches(x_hbm, x_ref, sems)
    pos = jnp.broadcast_to(pos_ref[0:1, :].astype(jnp.float32), (ROW, ROW)).astype(jnp.bfloat16)
    expand = onehot(iota((4 * ROW, ROW), 0) >> 2 == iota((4 * ROW, ROW), 1))
    slot = dot_nt(expand, pos).astype(jnp.int32)
    place_ref[...] = onehot(slot == iota((4 * ROW, ROW), 1))

    def chunk(i, carry):
        fetch(i).wait()
        for r in range(0, PART, 64):
            rows = pl.ds(pl.multiple_of(i * PART + r, 64), 64)
            acc = x_ref[0, rows, :].astype(jnp.float32) * scalars_ref[LEVELS : LEVELS + 1, :]
            for l in range(1, levels):
                acc = acc + x_ref[l, rows, :].astype(jnp.float32) * scalars_ref[LEVELS + l : LEVELS + l + 1, :]
            acc_ref[rows, :] = acc
        return carry

    lax.fori_loop(0, PARTS, chunk, 0)
    for k in range(2):
        sums_ref[pl.ds(k * ROW, ROW), :] = acc_ref[pl.ds(2 + k, ROW, stride=4), :]
    sums_ref[pl.ds(2 * ROW, 8), :] = scalars_ref[2 * LEVELS :, :]


def perturb_kernel(scalars_ref, arrived_ref, place_ref, x_hbm, y_hbm, clipped_ref, local_ref, x_ref, y_ref, in_sems, sems):
    levels = x_ref.shape[0]
    fetch = fetches(x_hbm, x_ref, in_sems)
    parts = three_parts(jnp.tanh(arrived_ref[...]))
    place = place_ref[...]
    local_ref[...] = (dot(place, parts[0]) + dot(place, parts[1])) + dot(place, parts[2])
    clipped_ref[...] = local_ref[pl.ds(0, ROW, stride=4), :]

    def store(i):
        rows = pl.ds(pl.multiple_of(i * PART, PART), PART)
        return pltpu.make_async_copy(y_ref.at[:, rows, :], y_hbm.at[:, rows, :], sems.at[i])

    def chunk(i, carry):
        fetch(i).wait()
        for r in range(0, PART, 32):
            rows = pl.ds(pl.multiple_of(i * PART + r, 32), 32)
            local = local_ref[rows, :]
            for l in range(levels):
                scale = 1.0 + scalars_ref[l : l + 1, :] * local
                y_ref[l, rows, :] = (x_ref[l, rows, :].astype(jnp.float32) * scale).astype(jnp.bfloat16)
        store(i).start()
        return carry

    lax.fori_loop(0, PARTS, chunk, 0)
    for i in range(PARTS):
        store(i).wait()


def integrals_kernel(local_ref, s0, s1, s2, s3, out_ref):
    local = local_ref[...]
    total = (s0[...] + s1[...]) + (s2[...] + s3[...])
    norm = jnp.sqrt(total[2 * ROW : 2 * ROW + 1, :])
    for k in range(2):
        out_ref[pl.ds(k, ROW, stride=2), :] = local * total[k * ROW : (k + 1) * ROW, :] / norm


def program(pattern, taper, thickness, block_source, tendencies):
    vmem, hbm = pl.BlockSpec(memory_space=pltpu.VMEM), pl.BlockSpec(memory_space=pltpu.HBM)
    levels = tendencies.shape[1]
    f32, s32 = jnp.float32, jnp.int32

    tables = [pattern] + [along_z(pattern, k) for k in (1, 2, 3)]
    scalar_rows = 2 * LEVELS + 8
    ids, pos, scalars = pl.pallas_call(
        request_kernel,
        out_shape=(
            jax.ShapeDtypeStruct((ROW, ROW), s32),
            jax.ShapeDtypeStruct((8, ROW), s32),
            jax.ShapeDtypeStruct((scalar_rows, ROW), f32),
        ),
        in_specs=[vmem, vmem, vmem],
        out_specs=(vmem, vmem, vmem),
        name="request",
    )(block_source.reshape(1, ROW), taper.reshape(1, levels), thickness.reshape(1, levels))
    wanted = within_plane(ids.reshape(16, 8, ROW)).reshape(ROW, ROW)

    x = tendencies.reshape(4, levels, ROW, ROW).transpose(1, 2, 0, 3).reshape(levels, 4 * ROW, ROW)
    sums, place = pl.pallas_call(
        column_kernel,
        out_shape=(jax.ShapeDtypeStruct((2 * ROW + 8, ROW), f32), jax.ShapeDtypeStruct((4 * ROW, ROW), jnp.bfloat16)),
        in_specs=[vmem, vmem, hbm],
        out_specs=(vmem, vmem),
        scratch_shapes=[
            pltpu.VMEM((4 * ROW, ROW), f32),
            pltpu.VMEM(x.shape, x.dtype),
            pltpu.SemaphoreType.DMA((PARTS,)),
        ],
        cost_estimate=pl.CostEstimate(flops=10_000_000, bytes_accessed=4_500_000, transcendentals=0),
        compiler_params=pltpu.CompilerParams(vmem_limit_bytes=52 << 20),
        name="columns",
    )(scalars, pos, x)
    others = [across_lev(sums, flip) for flip in (1, 2, 3)]

    picked = pl.pallas_call(
        pick_kernel,
        out_shape=jax.ShapeDtypeStruct((ROW, ROW), f32),
        in_specs=[vmem] * 5,
        out_specs=vmem,
        cost_estimate=pl.CostEstimate(flops=10_000_000, bytes_accessed=40_000_000, transcendentals=0),
        compiler_params=pltpu.CompilerParams(vmem_limit_bytes=4 << 20),
        name="pick",
    )(wanted, *tables)
    arrived = within_plane(picked.reshape(16, 8, ROW)).reshape(ROW, ROW)

    y, local = pl.pallas_call(
        perturb_kernel,
        out_shape=(jax.ShapeDtypeStruct(x.shape, x.dtype), jax.ShapeDtypeStruct((ROW, ROW), f32)),
        in_specs=[vmem, vmem, vmem, hbm],
        out_specs=(hbm, vmem),
        scratch_shapes=[
            pltpu.VMEM((4 * ROW, ROW), f32),
            pltpu.VMEM(x.shape, x.dtype),
            pltpu.VMEM(x.shape, x.dtype),
            pltpu.SemaphoreType.DMA((PARTS,)),
            pltpu.SemaphoreType.DMA((PARTS,)),
        ],
        cost_estimate=pl.CostEstimate(flops=10_000_000, bytes_accessed=9_000_000, transcendentals=0),
        compiler_params=pltpu.CompilerParams(vmem_limit_bytes=52 << 20),
        name="perturb",
    )(scalars, arrived, place, x)
    out = pl.pallas_call(
        integrals_kernel,
        out_shape=jax.ShapeDtypeStruct((2 * ROW, ROW), f32),
        in_specs=[vmem] * 5,
        out_specs=vmem,
        compiler_params=pltpu.CompilerParams(vmem_limit_bytes=4 << 20),
        name="integrals",
    )(local, sums, *others)
    perturbed = y.reshape(levels, ROW, 4, ROW).transpose(2, 0, 1, 3).reshape(tendencies.shape)
    integrals = out.reshape(ROW, 2, ROW).transpose(1, 0, 2).reshape(2, ROW * ROW)
    return perturbed, integrals


def solution(mesh):
    split = jax.sharding.Mesh(mesh.devices.reshape(4, 4, 4, 4), ("x", "z", "y", "lev"))
    band = ("x", "z", "y")
    in_specs = (P(band, None), P("lev"), P("lev"), P(band), P(None, "lev", band))
    out_specs = (P(None, "lev", band), P(None, band))
    return jax.shard_map(program, mesh=split, in_specs=in_specs, out_specs=out_specs, check_vma=False)
```

```python
import jax
import jax.numpy as jnp
from jax import lax
from jax.experimental import pallas as pl
from jax.experimental.pallas import tpu as pltpu
from jax.sharding import PartitionSpec as P


OFFSET = (0, 3, 1, 2)
SOURCE = (0, 2, 1, 3)
ROW = 128
LEVELS = 40
PARTS = 8
PART = 4 * ROW // PARTS


def along_z(a):
    pairs = []
    for z in range(4):
        for lev in range(4):
            pairs.append((((z + OFFSET[lev]) % 4) * 4 + SOURCE[lev], z * 4 + lev))
    return lax.ppermute(a, ("z", "lev"), pairs)


def across_lev(a, flip):
    return lax.ppermute(a, "lev", [(i, i ^ flip) for i in range(4)])


def iota(shape, dim):
    return lax.broadcasted_iota(jnp.int32, shape, dim)


def onehot(cond):
    return jnp.where(cond, 1.0, 0.0).astype(jnp.bfloat16)


def dot(a, b):
    return jnp.dot(a, b, preferred_element_type=jnp.float32)


def dot_nt(a, b):
    return lax.dot_general(a, b, (((1,), (1,)), ((), ())), preferred_element_type=jnp.float32)


def three_parts(v):
    high = v.astype(jnp.bfloat16)
    rest = v - high.astype(jnp.float32)
    mid = rest.astype(jnp.bfloat16)
    low = (rest - mid.astype(jnp.float32)).astype(jnp.bfloat16)
    return high, mid, low


def request_kernel(source_ref, taper_ref, thick_ref, ids_ref, scalars_ref):
    source = source_ref[...]
    band, row = source >> 7, source & 127
    offset = ((band >> 2) - lax.axis_index("z")) & 3
    lev = jnp.where(offset == 3, 1, jnp.where(offset == 0, 0, offset + 1))
    holder = ((band >> 4) * 4 + (band & 3)) * 4 + lev
    member = iota((64, ROW), 0) == holder
    before = onehot(iota((ROW, ROW), 0) < iota((ROW, ROW), 1))
    count = dot(onehot(member), before)
    rank = jnp.sum(jnp.where(member, count, 0.0), axis=0, keepdims=True)
    pos = holder * 2 + rank.astype(jnp.int32)
    slot = iota((ROW, ROW), 0)
    asked = (slot >> 3) * 8 + lax.axis_index("lev") * 2 + (slot & 1)
    rows = jnp.broadcast_to(row.astype(jnp.float32), (ROW, ROW)).astype(jnp.bfloat16)
    ids_ref[...] = dot_nt(onehot(asked == pos), rows).astype(jnp.int32)

    taper, thick = taper_ref[...], thick_ref[...]
    levels = taper.shape[1]
    diagonal = iota((LEVELS, levels), 0) == iota((LEVELS, levels), 1)

    def one_per_row(v):
        total = jnp.sum(jnp.where(diagonal, jnp.broadcast_to(v, diagonal.shape), 0.0), axis=1, keepdims=True)
        return jnp.broadcast_to(total, (LEVELS, ROW))

    scalars_ref[0:LEVELS, :] = one_per_row(taper)
    scalars_ref[LEVELS : 2 * LEVELS, :] = one_per_row(taper * thick)
    scalars_ref[2 * LEVELS : 2 * LEVELS + 8, :] = jnp.broadcast_to(jnp.sum(thick * thick, axis=1, keepdims=True), (8, ROW))
    scalars_ref[2 * LEVELS + 8 :, :] = jnp.broadcast_to(pos.astype(jnp.float32), (8, ROW))


def pick_kernel(ids_ref, table_ref, out_ref):
    pick = onehot(ids_ref[...] == iota((ROW, ROW), 1))
    high, mid, low = three_parts(table_ref[...])
    out_ref[...] = (dot(pick, high) + dot(pick, mid)) + dot(pick, low)


def fetches(x_hbm, x_ref, sems):
    def fetch(i):
        rows = pl.ds(pl.multiple_of(i * PART, PART), PART)
        return pltpu.make_async_copy(x_hbm.at[:, rows, :], x_ref.at[:, rows, :], sems.at[i])

    for i in range(PARTS):
        fetch(i).start()
    return fetch


def column_kernel(scalars_ref, x_hbm, sums_ref, place_ref, acc_ref, x_ref, sems):
    levels = x_ref.shape[0]
    fetch = fetches(x_hbm, x_ref, sems)
    pos = jnp.broadcast_to(scalars_ref[2 * LEVELS + 8 : 2 * LEVELS + 9, :], (ROW, ROW)).astype(jnp.bfloat16)
    expand = onehot(iota((4 * ROW, ROW), 0) >> 2 == iota((4 * ROW, ROW), 1))
    slot = dot_nt(expand, pos).astype(jnp.int32)
    place_ref[...] = onehot(slot == iota((4 * ROW, ROW), 1))

    def chunk(i, carry):
        fetch(i).wait()
        for r in range(0, PART, 64):
            rows = pl.ds(pl.multiple_of(i * PART + r, 64), 64)
            acc = x_ref[0, rows, :].astype(jnp.float32) * scalars_ref[LEVELS : LEVELS + 1, :]
            for l in range(1, levels):
                acc = acc + x_ref[l, rows, :].astype(jnp.float32) * scalars_ref[LEVELS + l : LEVELS + l + 1, :]
            acc_ref[rows, :] = acc
        return carry

    lax.fori_loop(0, PARTS, chunk, 0)
    for k in range(2):
        sums_ref[pl.ds(k * ROW, ROW), :] = acc_ref[pl.ds(2 + k, ROW, stride=4), :]
    sums_ref[pl.ds(2 * ROW, 8), :] = scalars_ref[2 * LEVELS : 2 * LEVELS + 8, :]


def perturb_kernel(scalars_ref, arrived_ref, place_ref, x_hbm, y_hbm, clipped_ref, local_ref, x_ref, y_ref, in_sems, sems):
    levels = x_ref.shape[0]
    fetch = fetches(x_hbm, x_ref, in_sems)
    parts = three_parts(jnp.tanh(arrived_ref[...]))
    place = place_ref[...]
    local_ref[...] = (dot(place, parts[0]) + dot(place, parts[1])) + dot(place, parts[2])

    def store(i):
        rows = pl.ds(pl.multiple_of(i * PART, PART), PART)
        return pltpu.make_async_copy(y_ref.at[:, rows, :], y_hbm.at[:, rows, :], sems.at[i])

    def chunk(i, carry):
        fetch(i).wait()
        for r in range(0, PART, 32):
            rows = pl.ds(pl.multiple_of(i * PART + r, 32), 32)
            local = local_ref[rows, :]
            for l in range(levels):
                scale = 1.0 + scalars_ref[l : l + 1, :] * local
                y_ref[l, rows, :] = (x_ref[l, rows, :].astype(jnp.float32) * scale).astype(jnp.bfloat16)
        store(i).start()
        return carry

    lax.fori_loop(0, PARTS, chunk, 0)

    clipped_ref[...] = local_ref[pl.ds(0, ROW, stride=4), :]
    for i in range(PARTS):
        store(i).wait()


def integrals_kernel(local_ref, s0, s1, s2, s3, out_ref):
    local = local_ref[...]
    total = (s0[...] + s1[...]) + (s2[...] + s3[...])
    norm = jnp.sqrt(total[2 * ROW : 2 * ROW + 1, :])
    for k in range(2):
        out_ref[pl.ds(k, ROW, stride=2), :] = local * total[k * ROW : (k + 1) * ROW, :] / norm


def program(pattern, taper, thickness, block_source, tendencies):
    vmem, hbm = pl.BlockSpec(memory_space=pltpu.VMEM), pl.BlockSpec(memory_space=pltpu.HBM)
    levels = tendencies.shape[1]
    f32, s32 = jnp.float32, jnp.int32

    table = along_z(pattern)
    ids, scalars = pl.pallas_call(
        request_kernel,
        out_shape=(jax.ShapeDtypeStruct((ROW, ROW), s32), jax.ShapeDtypeStruct((2 * LEVELS + 16, ROW), f32)),
        in_specs=[vmem, vmem, vmem],
        out_specs=(vmem, vmem),
        name="request",
    )(block_source.reshape(1, ROW), taper.reshape(1, levels), thickness.reshape(1, levels))
    wanted = lax.all_to_all(ids.reshape(16, 8, ROW), ("x", "y"), 0, 0, tiled=True).reshape(ROW, ROW)

    x = tendencies.reshape(4, levels, ROW, ROW).transpose(1, 2, 0, 3).reshape(levels, 4 * ROW, ROW)
    sums, place = pl.pallas_call(
        column_kernel,
        out_shape=(jax.ShapeDtypeStruct((2 * ROW + 8, ROW), f32), jax.ShapeDtypeStruct((4 * ROW, ROW), jnp.bfloat16)),
        in_specs=[vmem, hbm],
        out_specs=(vmem, vmem),
        scratch_shapes=[
            pltpu.VMEM((4 * ROW, ROW), f32),
            pltpu.VMEM(x.shape, x.dtype),
            pltpu.SemaphoreType.DMA((PARTS,)),
        ],
        cost_estimate=pl.CostEstimate(flops=10_000_000, bytes_accessed=4_500_000, transcendentals=0),
        compiler_params=pltpu.CompilerParams(vmem_limit_bytes=52 << 20),
        name="columns",
    )(scalars, x)
    others = [across_lev(sums, flip) for flip in (1, 2, 3)]

    picked = pl.pallas_call(
        pick_kernel,
        out_shape=jax.ShapeDtypeStruct((ROW, ROW), f32),
        in_specs=[vmem] * 2,
        out_specs=vmem,
        compiler_params=pltpu.CompilerParams(vmem_limit_bytes=4 << 20),
        name="pick",
    )(wanted, table)
    arrived = lax.all_to_all(picked.reshape(64, 2, ROW), ("x", "y", "lev"), 0, 0, tiled=True).reshape(ROW, ROW)

    y, local = pl.pallas_call(
        perturb_kernel,
        out_shape=(jax.ShapeDtypeStruct(x.shape, x.dtype), jax.ShapeDtypeStruct((ROW, ROW), f32)),
        in_specs=[vmem, vmem, vmem, hbm],
        out_specs=(hbm, vmem),
        scratch_shapes=[
            pltpu.VMEM((4 * ROW, ROW), f32),
            pltpu.VMEM(x.shape, x.dtype),
            pltpu.VMEM(x.shape, x.dtype),
            pltpu.SemaphoreType.DMA((PARTS,)),
            pltpu.SemaphoreType.DMA((PARTS,)),
        ],
        cost_estimate=pl.CostEstimate(flops=10_000_000, bytes_accessed=9_000_000, transcendentals=0),
        compiler_params=pltpu.CompilerParams(vmem_limit_bytes=52 << 20),
        name="perturb",
    )(scalars, arrived, place, x)
    out = pl.pallas_call(
        integrals_kernel,
        out_shape=jax.ShapeDtypeStruct((2 * ROW, ROW), f32),
        in_specs=[vmem] * 5,
        out_specs=vmem,
        compiler_params=pltpu.CompilerParams(vmem_limit_bytes=4 << 20),
        name="integrals",
    )(local, sums, *others)
    perturbed = y.reshape(levels, ROW, 4, ROW).transpose(2, 0, 1, 3).reshape(tendencies.shape)
    integrals = out.reshape(ROW, 2, ROW).transpose(1, 0, 2).reshape(2, ROW * ROW)
    return perturbed, integrals


def solution(mesh):
    split = jax.sharding.Mesh(mesh.devices.reshape(4, 4, 4, 4), ("x", "z", "y", "lev"))
    band = ("x", "z", "y")
    in_specs = (P(band, None), P("lev"), P("lev"), P(band), P(None, "lev", band))
    out_specs = (P(None, "lev", band), P(None, band))
    return jax.shard_map(program, mesh=split, in_specs=in_specs, out_specs=out_specs, check_vma=False)
```

```python
import jax
import jax.numpy as jnp
from jax import lax
from jax.experimental import pallas as pl
from jax.experimental.pallas import tpu as pltpu
from jax.sharding import PartitionSpec as P


OFFSET = (0, 3, 1, 2)
SOURCE = (0, 2, 1, 3)
ROW = 128
LEVELS = 40
PARTS = 8
PART = 4 * ROW // PARTS


def along_z(a):
    pairs = []
    for z in range(4):
        for lev in range(4):
            pairs.append((((z + OFFSET[lev]) % 4) * 4 + SOURCE[lev], z * 4 + lev))
    return lax.ppermute(a, ("z", "lev"), pairs)


def along_y(a, step):
    return lax.ppermute(a, "y", [(y, (y + step) % 4) for y in range(4)])


def across_lev(a, flip):
    return lax.ppermute(a, "lev", [(i, i ^ flip) for i in range(4)])


def iota(shape, dim):
    return lax.broadcasted_iota(jnp.int32, shape, dim)


def onehot(cond):
    return jnp.where(cond, 1.0, 0.0).astype(jnp.bfloat16)


def dot(a, b):
    return jnp.dot(a, b, preferred_element_type=jnp.float32)


def dot_nt(a, b):
    return lax.dot_general(a, b, (((1,), (1,)), ((), ())), preferred_element_type=jnp.float32)


def three_parts(v):
    high = v.astype(jnp.bfloat16)
    rest = v - high.astype(jnp.float32)
    mid = rest.astype(jnp.bfloat16)
    low = (rest - mid.astype(jnp.float32)).astype(jnp.bfloat16)
    return high, mid, low


def request_kernel(source_ref, taper_ref, thick_ref, ids_ref, scalars_ref):
    source = source_ref[...]
    band, row = source >> 7, source & 127
    offset = ((band >> 2) - lax.axis_index("z")) & 3
    lev = jnp.where(offset == 3, 1, jnp.where(offset == 0, 0, offset + 1))
    table = (lax.axis_index("y") - band) & 3
    holder = ((band >> 4) * 4 + lev) * 4 + table
    member = iota((64, ROW), 0) == holder
    before = onehot(iota((ROW, ROW), 0) < iota((ROW, ROW), 1))
    count = dot(onehot(member), before)
    rank = jnp.sum(jnp.where(member, count, 0.0), axis=0, keepdims=True)
    pos = holder * 2 + rank.astype(jnp.int32)
    slot = iota((ROW, ROW), 0)
    asked = onehot(((slot >> 5) * 4 + lax.axis_index("lev")) * 8 + (slot & 7) == pos)

    def everywhere(v):
        return jnp.broadcast_to(v.astype(jnp.float32), (ROW, ROW)).astype(jnp.bfloat16)

    ids = dot_nt(asked, everywhere(table)) * 128.0 + dot_nt(asked, everywhere(row))
    ids_ref[...] = ids.astype(jnp.int32)

    taper, thick = taper_ref[...], thick_ref[...]
    levels = taper.shape[1]
    diagonal = iota((LEVELS, levels), 0) == iota((LEVELS, levels), 1)

    def one_per_row(v):
        total = jnp.sum(jnp.where(diagonal, jnp.broadcast_to(v, diagonal.shape), 0.0), axis=1, keepdims=True)
        return jnp.broadcast_to(total, (LEVELS, ROW))

    scalars_ref[0:LEVELS, :] = one_per_row(taper)
    scalars_ref[LEVELS : 2 * LEVELS, :] = one_per_row(taper * thick)
    scalars_ref[2 * LEVELS : 2 * LEVELS + 8, :] = jnp.broadcast_to(jnp.sum(thick * thick, axis=1, keepdims=True), (8, ROW))
    scalars_ref[2 * LEVELS + 8 :, :] = jnp.broadcast_to(pos.astype(jnp.float32), (8, ROW))


def pick_kernel(ids_ref, t0, t1, t2, t3, out_ref):
    ids, lane = ids_ref[...], iota((ROW, ROW), 1)
    total = None
    for c, ref in enumerate((t0, t1, t2, t3)):
        pick = onehot(ids == lane + c * ROW)
        part = tuple(dot(pick, v) for v in three_parts(ref[...]))
        total = part if total is None else tuple(a + b for a, b in zip(total, part))
    out_ref[...] = (total[0] + total[1]) + total[2]


def fetches(x_hbm, x_ref, sems):
    def fetch(i):
        rows = pl.ds(pl.multiple_of(i * PART, PART), PART)
        return pltpu.make_async_copy(x_hbm.at[:, rows, :], x_ref.at[:, rows, :], sems.at[i])

    for i in range(PARTS):
        fetch(i).start()
    return fetch


def column_kernel(scalars_ref, x_hbm, sums_ref, place_ref, acc_ref, x_ref, sems):
    levels = x_ref.shape[0]
    fetch = fetches(x_hbm, x_ref, sems)
    pos = jnp.broadcast_to(scalars_ref[2 * LEVELS + 8 : 2 * LEVELS + 9, :], (ROW, ROW)).astype(jnp.bfloat16)
    expand = onehot(iota((4 * ROW, ROW), 0) >> 2 == iota((4 * ROW, ROW), 1))
    slot = dot_nt(expand, pos).astype(jnp.int32)
    place_ref[...] = onehot(slot == iota((4 * ROW, ROW), 1))

    def chunk(i, carry):
        fetch(i).wait()
        for r in range(0, PART, 64):
            rows = pl.ds(pl.multiple_of(i * PART + r, 64), 64)
            acc = x_ref[0, rows, :].astype(jnp.float32) * scalars_ref[LEVELS : LEVELS + 1, :]
            for l in range(1, levels):
                acc = acc + x_ref[l, rows, :].astype(jnp.float32) * scalars_ref[LEVELS + l : LEVELS + l + 1, :]
            acc_ref[rows, :] = acc
        return carry

    lax.fori_loop(0, PARTS, chunk, 0)
    for k in range(2):
        sums_ref[pl.ds(k * ROW, ROW), :] = acc_ref[pl.ds(2 + k, ROW, stride=4), :]
    sums_ref[pl.ds(2 * ROW, 8), :] = scalars_ref[2 * LEVELS : 2 * LEVELS + 8, :]


def perturb_kernel(scalars_ref, arrived_ref, place_ref, x_hbm, y_hbm, clipped_ref, local_ref, x_ref, y_ref, in_sems, sems):
    levels = x_ref.shape[0]
    fetch = fetches(x_hbm, x_ref, in_sems)
    parts = three_parts(jnp.tanh(arrived_ref[...]))
    place = place_ref[...]
    local_ref[...] = (dot(place, parts[0]) + dot(place, parts[1])) + dot(place, parts[2])

    def store(i):
        rows = pl.ds(pl.multiple_of(i * PART, PART), PART)
        return pltpu.make_async_copy(y_ref.at[:, rows, :], y_hbm.at[:, rows, :], sems.at[i])

    def chunk(i, carry):
        fetch(i).wait()
        for r in range(0, PART, 32):
            rows = pl.ds(pl.multiple_of(i * PART + r, 32), 32)
            local = local_ref[rows, :]
            for l in range(levels):
                scale = 1.0 + scalars_ref[l : l + 1, :] * local
                y_ref[l, rows, :] = (x_ref[l, rows, :].astype(jnp.float32) * scale).astype(jnp.bfloat16)
        store(i).start()
        return carry

    lax.fori_loop(0, PARTS, chunk, 0)

    clipped_ref[...] = local_ref[pl.ds(0, ROW, stride=4), :]
    for i in range(PARTS):
        store(i).wait()


def integrals_kernel(local_ref, s0, s1, s2, s3, out_ref):
    local = local_ref[...]
    total = (s0[...] + s1[...]) + (s2[...] + s3[...])
    norm = jnp.sqrt(total[2 * ROW : 2 * ROW + 1, :])
    for k in range(2):
        out_ref[pl.ds(k, ROW, stride=2), :] = local * total[k * ROW : (k + 1) * ROW, :] / norm


def program(pattern, taper, thickness, block_source, tendencies):
    vmem, hbm = pl.BlockSpec(memory_space=pltpu.VMEM), pl.BlockSpec(memory_space=pltpu.HBM)
    levels = tendencies.shape[1]
    f32, s32 = jnp.float32, jnp.int32

    table = along_z(pattern)
    ids, scalars = pl.pallas_call(
        request_kernel,
        out_shape=(jax.ShapeDtypeStruct((ROW, ROW), s32), jax.ShapeDtypeStruct((2 * LEVELS + 16, ROW), f32)),
        in_specs=[vmem, vmem, vmem],
        out_specs=(vmem, vmem),
        name="request",
    )(block_source.reshape(1, ROW), taper.reshape(1, levels), thickness.reshape(1, levels))
    wanted = lax.all_to_all(ids.reshape(4, 32, ROW), "x", 0, 0, tiled=True).reshape(ROW, ROW)
    tables = [table] + [along_y(table, k) for k in (1, 2, 3)]

    x = tendencies.reshape(4, levels, ROW, ROW).transpose(1, 2, 0, 3).reshape(levels, 4 * ROW, ROW)
    sums, place = pl.pallas_call(
        column_kernel,
        out_shape=(jax.ShapeDtypeStruct((2 * ROW + 8, ROW), f32), jax.ShapeDtypeStruct((4 * ROW, ROW), jnp.bfloat16)),
        in_specs=[vmem, hbm],
        out_specs=(vmem, vmem),
        scratch_shapes=[
            pltpu.VMEM((4 * ROW, ROW), f32),
            pltpu.VMEM(x.shape, x.dtype),
            pltpu.SemaphoreType.DMA((PARTS,)),
        ],
        cost_estimate=pl.CostEstimate(flops=10_000_000, bytes_accessed=4_500_000, transcendentals=0),
        compiler_params=pltpu.CompilerParams(vmem_limit_bytes=52 << 20),
        name="columns",
    )(scalars, x)
    others = [across_lev(sums, flip) for flip in (1, 2, 3)]

    picked = pl.pallas_call(
        pick_kernel,
        out_shape=jax.ShapeDtypeStruct((ROW, ROW), f32),
        in_specs=[vmem] * 5,
        out_specs=vmem,
        compiler_params=pltpu.CompilerParams(vmem_limit_bytes=4 << 20),
        name="pick",
    )(wanted, *tables)
    arrived = lax.all_to_all(picked.reshape(16, 8, ROW), ("x", "lev"), 0, 0, tiled=True).reshape(ROW, ROW)

    y, local = pl.pallas_call(
        perturb_kernel,
        out_shape=(jax.ShapeDtypeStruct(x.shape, x.dtype), jax.ShapeDtypeStruct((ROW, ROW), f32)),
        in_specs=[vmem, vmem, vmem, hbm],
        out_specs=(hbm, vmem),
        scratch_shapes=[
            pltpu.VMEM((4 * ROW, ROW), f32),
            pltpu.VMEM(x.shape, x.dtype),
            pltpu.VMEM(x.shape, x.dtype),
            pltpu.SemaphoreType.DMA((PARTS,)),
            pltpu.SemaphoreType.DMA((PARTS,)),
        ],
        cost_estimate=pl.CostEstimate(flops=10_000_000, bytes_accessed=9_000_000, transcendentals=0),
        compiler_params=pltpu.CompilerParams(vmem_limit_bytes=52 << 20),
        name="perturb",
    )(scalars, arrived, place, x)
    out = pl.pallas_call(
        integrals_kernel,
        out_shape=jax.ShapeDtypeStruct((2 * ROW, ROW), f32),
        in_specs=[vmem] * 5,
        out_specs=vmem,
        compiler_params=pltpu.CompilerParams(vmem_limit_bytes=4 << 20),
        name="integrals",
    )(local, sums, *others)
    perturbed = y.reshape(levels, ROW, 4, ROW).transpose(2, 0, 1, 3).reshape(tendencies.shape)
    integrals = out.reshape(ROW, 2, ROW).transpose(1, 0, 2).reshape(2, ROW * ROW)
    return perturbed, integrals


def solution(mesh):
    split = jax.sharding.Mesh(mesh.devices.reshape(4, 4, 4, 4), ("x", "z", "y", "lev"))
    band = ("x", "z", "y")
    in_specs = (P(band, None), P("lev"), P("lev"), P(band), P(None, "lev", band))
    out_specs = (P(None, "lev", band), P(None, band))
    return jax.shard_map(program, mesh=split, in_specs=in_specs, out_specs=out_specs, check_vma=False)
```

```python
import jax
import jax.numpy as jnp
from jax import lax
from jax.experimental import pallas as pl
from jax.experimental.pallas import tpu as pltpu
from jax.sharding import PartitionSpec as P


OFFSET = (0, 3, 1, 2)
SOURCE = (0, 2, 1, 3)
ROW = 128
LEVELS = 40
PARTS = 8
PART = 4 * ROW // PARTS


def along_z(a):
    pairs = []
    for z in range(4):
        for lev in range(4):
            pairs.append((((z + OFFSET[lev]) % 4) * 4 + SOURCE[lev], z * 4 + lev))
    return lax.ppermute(a, ("z", "lev"), pairs)


def along_y(a, step):
    return lax.ppermute(a, "y", [(y, (y + step) % 4) for y in range(4)])


def along_x(a, step):
    return lax.ppermute(a, "x", [(x, (x + step) % 4) for x in range(4)])


def across_lev(a, flip):
    return lax.ppermute(a, "lev", [(i, i ^ flip) for i in range(4)])


def iota(shape, dim):
    return lax.broadcasted_iota(jnp.int32, shape, dim)


def onehot(cond):
    return jnp.where(cond, 1.0, 0.0).astype(jnp.bfloat16)


def dot(a, b):
    return jnp.dot(a, b, preferred_element_type=jnp.float32)


def dot_nt(a, b):
    return lax.dot_general(a, b, (((1,), (1,)), ((), ())), preferred_element_type=jnp.float32)


def three_parts(v):
    high = v.astype(jnp.bfloat16)
    rest = v - high.astype(jnp.float32)
    mid = rest.astype(jnp.bfloat16)
    low = (rest - mid.astype(jnp.float32)).astype(jnp.bfloat16)
    return high, mid, low


def parts_of(source):
    band, row = source >> 7, source & 127
    offset = ((band >> 2) - lax.axis_index("z")) & 3
    lev = jnp.where(offset == 3, 1, jnp.where(offset == 0, 0, offset + 1))
    return band >> 4, lev, (lax.axis_index("y") - band) & 3, row


def prepare_kernel(source_ref, taper_ref, thick_ref, scalars_ref):
    source = source_ref[...]
    x, lev, table, _ = parts_of(source)
    holder = (x * 4 + lev) * 4 + table
    member = iota((64, ROW), 0) == holder
    before = onehot(iota((ROW, ROW), 0) < iota((ROW, ROW), 1))
    count = dot(onehot(member), before)
    rank = jnp.sum(jnp.where(member, count, 0.0), axis=0, keepdims=True)
    pos = holder * 2 + rank.astype(jnp.int32)

    taper, thick = taper_ref[...], thick_ref[...]
    levels = taper.shape[1]
    diagonal = iota((LEVELS, levels), 0) == iota((LEVELS, levels), 1)

    def one_per_row(v):
        total = jnp.sum(jnp.where(diagonal, jnp.broadcast_to(v, diagonal.shape), 0.0), axis=1, keepdims=True)
        return jnp.broadcast_to(total, (LEVELS, ROW))

    scalars_ref[0:LEVELS, :] = one_per_row(taper)
    scalars_ref[LEVELS : 2 * LEVELS, :] = one_per_row(taper * thick)
    scalars_ref[2 * LEVELS : 2 * LEVELS + 8, :] = jnp.broadcast_to(jnp.sum(thick * thick, axis=1, keepdims=True), (8, ROW))
    scalars_ref[2 * LEVELS + 8 : 2 * LEVELS + 16, :] = jnp.broadcast_to(pos.astype(jnp.float32), (8, ROW))
    scalars_ref[2 * LEVELS + 16 :, :] = jnp.broadcast_to(source.astype(jnp.float32), (8, ROW))


def wanted_kernel(scalars_ref, from1, from2, from3, ids_ref):
    slot = iota((ROW, ROW), 0)
    step = (lax.axis_index("x") - (slot >> 5)) & 3
    own = scalars_ref[2 * LEVELS + 16 : 2 * LEVELS + 17, :].astype(jnp.int32)
    source = jnp.where(step == 0, own, jnp.where(step == 1, from1[...], jnp.where(step == 2, from2[...], from3[...])))
    x, lev, table, row = parts_of(source)
    mine = (x == lax.axis_index("x")) & (lev == lax.axis_index("lev")) & (table == ((slot >> 1) & 3))
    before = onehot(iota((ROW, ROW), 0) < iota((ROW, ROW), 1))
    count = dot(onehot(mine), before)
    chosen = mine & (count == (slot & 1).astype(jnp.float32))
    ids = jnp.sum(jnp.where(chosen, (table * ROW + row).astype(jnp.float32), 0.0), axis=1, keepdims=True)
    ids_ref[...] = jnp.broadcast_to(ids, (ROW, ROW)).astype(jnp.int32)


def pick_kernel(ids_ref, t0, t1, t2, t3, out_ref):
    ids, lane = ids_ref[...], iota((ROW, ROW), 1)
    total = None
    for c, ref in enumerate((t0, t1, t2, t3)):
        pick = onehot(ids == lane + c * ROW)
        part = tuple(dot(pick, v) for v in three_parts(ref[...]))
        total = part if total is None else tuple(a + b for a, b in zip(total, part))
    out_ref[...] = (total[0] + total[1]) + total[2]


def fetches(x_hbm, x_ref, sems):
    def fetch(i):
        rows = pl.ds(pl.multiple_of(i * PART, PART), PART)
        return pltpu.make_async_copy(x_hbm.at[:, rows, :], x_ref.at[:, rows, :], sems.at[i])

    for i in range(PARTS):
        fetch(i).start()
    return fetch


def column_kernel(scalars_ref, x_hbm, sums_ref, place_ref, acc_ref, x_ref, sems):
    levels = x_ref.shape[0]
    fetch = fetches(x_hbm, x_ref, sems)
    pos = jnp.broadcast_to(scalars_ref[2 * LEVELS + 8 : 2 * LEVELS + 9, :], (ROW, ROW)).astype(jnp.bfloat16)
    expand = onehot(iota((4 * ROW, ROW), 0) >> 2 == iota((4 * ROW, ROW), 1))
    slot = dot_nt(expand, pos).astype(jnp.int32)
    place_ref[...] = onehot(slot == iota((4 * ROW, ROW), 1))

    def chunk(i, carry):
        fetch(i).wait()
        for r in range(0, PART, 64):
            rows = pl.ds(pl.multiple_of(i * PART + r, 64), 64)
            acc = x_ref[0, rows, :].astype(jnp.float32) * scalars_ref[LEVELS : LEVELS + 1, :]
            for l in range(1, levels):
                acc = acc + x_ref[l, rows, :].astype(jnp.float32) * scalars_ref[LEVELS + l : LEVELS + l + 1, :]
            acc_ref[rows, :] = acc
        return carry

    lax.fori_loop(0, PARTS, chunk, 0)
    for k in range(2):
        sums_ref[pl.ds(k * ROW, ROW), :] = acc_ref[pl.ds(2 + k, ROW, stride=4), :]
    sums_ref[pl.ds(2 * ROW, 8), :] = scalars_ref[2 * LEVELS : 2 * LEVELS + 8, :]


def perturb_kernel(scalars_ref, arrived_ref, place_ref, x_hbm, y_hbm, clipped_ref, local_ref, x_ref, y_ref, in_sems, sems):
    levels = x_ref.shape[0]
    fetch = fetches(x_hbm, x_ref, in_sems)
    parts = three_parts(jnp.tanh(arrived_ref[...]))
    place = place_ref[...]
    local_ref[...] = (dot(place, parts[0]) + dot(place, parts[1])) + dot(place, parts[2])

    def store(i):
        rows = pl.ds(pl.multiple_of(i * PART, PART), PART)
        return pltpu.make_async_copy(y_ref.at[:, rows, :], y_hbm.at[:, rows, :], sems.at[i])

    def chunk(i, carry):
        fetch(i).wait()
        for r in range(0, PART, 32):
            rows = pl.ds(pl.multiple_of(i * PART + r, 32), 32)
            local = local_ref[rows, :]
            for l in range(levels):
                scale = 1.0 + scalars_ref[l : l + 1, :] * local
                y_ref[l, rows, :] = (x_ref[l, rows, :].astype(jnp.float32) * scale).astype(jnp.bfloat16)
        store(i).start()
        return carry

    lax.fori_loop(0, PARTS, chunk, 0)

    clipped_ref[...] = local_ref[pl.ds(0, ROW, stride=4), :]
    for i in range(PARTS):
        store(i).wait()


def add_kernel(a_ref, b_ref, out_ref):
    out_ref[...] = a_ref[...] + b_ref[...]


def integrals_kernel(local_ref, s0, s1, out_ref):
    local = local_ref[...]
    total = s0[...] + s1[...]
    norm = jnp.sqrt(total[2 * ROW : 2 * ROW + 1, :])
    for k in range(2):
        out_ref[pl.ds(k, ROW, stride=2), :] = local * total[k * ROW : (k + 1) * ROW, :] / norm


def program(pattern, taper, thickness, block_source, tendencies):
    vmem, hbm = pl.BlockSpec(memory_space=pltpu.VMEM), pl.BlockSpec(memory_space=pltpu.HBM)
    levels = tendencies.shape[1]
    f32, s32 = jnp.float32, jnp.int32

    table = along_z(pattern)
    source = block_source.reshape(1, ROW)
    asked = [along_x(source, k) for k in (1, 2, 3)]
    scalars = pl.pallas_call(
        prepare_kernel,
        out_shape=jax.ShapeDtypeStruct((2 * LEVELS + 24, ROW), f32),
        in_specs=[vmem] * 3,
        out_specs=vmem,
        name="prepare",
    )(source, taper.reshape(1, levels), thickness.reshape(1, levels))
    tables = [table] + [along_y(table, k) for k in (1, 2, 3)]
    wanted = pl.pallas_call(
        wanted_kernel,
        out_shape=jax.ShapeDtypeStruct((ROW, ROW), s32),
        in_specs=[vmem] * 4,
        out_specs=vmem,
        compiler_params=pltpu.CompilerParams(vmem_limit_bytes=4 << 20),
        name="wanted",
    )(scalars, *asked)

    x = tendencies.reshape(4, levels, ROW, ROW).transpose(1, 2, 0, 3).reshape(levels, 4 * ROW, ROW)
    sums, place = pl.pallas_call(
        column_kernel,
        out_shape=(jax.ShapeDtypeStruct((2 * ROW + 8, ROW), f32), jax.ShapeDtypeStruct((4 * ROW, ROW), jnp.bfloat16)),
        in_specs=[vmem, hbm],
        out_specs=(vmem, vmem),
        scratch_shapes=[
            pltpu.VMEM((4 * ROW, ROW), f32),
            pltpu.VMEM(x.shape, x.dtype),
            pltpu.SemaphoreType.DMA((PARTS,)),
        ],
        cost_estimate=pl.CostEstimate(flops=10_000_000, bytes_accessed=4_500_000, transcendentals=0),
        compiler_params=pltpu.CompilerParams(vmem_limit_bytes=52 << 20),
        name="columns",
    )(scalars, x)
    pair = across_lev(sums, 1)
    both = pl.pallas_call(
        add_kernel,
        out_shape=jax.ShapeDtypeStruct(sums.shape, f32),
        in_specs=[vmem] * 2,
        out_specs=vmem,
        compiler_params=pltpu.CompilerParams(vmem_limit_bytes=4 << 20),
        name="both",
    )(sums, pair)
    rest = across_lev(both, 2)

    picked = pl.pallas_call(
        pick_kernel,
        out_shape=jax.ShapeDtypeStruct((ROW, ROW), f32),
        in_specs=[vmem] * 5,
        out_specs=vmem,
        compiler_params=pltpu.CompilerParams(vmem_limit_bytes=4 << 20),
        name="pick",
    )(wanted, *tables)
    arrived = lax.all_to_all(picked.reshape(16, 8, ROW), ("x", "lev"), 0, 0, tiled=True).reshape(ROW, ROW)

    y, local = pl.pallas_call(
        perturb_kernel,
        out_shape=(jax.ShapeDtypeStruct(x.shape, x.dtype), jax.ShapeDtypeStruct((ROW, ROW), f32)),
        in_specs=[vmem, vmem, vmem, hbm],
        out_specs=(hbm, vmem),
        scratch_shapes=[
            pltpu.VMEM((4 * ROW, ROW), f32),
            pltpu.VMEM(x.shape, x.dtype),
            pltpu.VMEM(x.shape, x.dtype),
            pltpu.SemaphoreType.DMA((PARTS,)),
            pltpu.SemaphoreType.DMA((PARTS,)),
        ],
        cost_estimate=pl.CostEstimate(flops=10_000_000, bytes_accessed=9_000_000, transcendentals=0),
        compiler_params=pltpu.CompilerParams(vmem_limit_bytes=52 << 20),
        name="perturb",
    )(scalars, arrived, place, x)
    out = pl.pallas_call(
        integrals_kernel,
        out_shape=jax.ShapeDtypeStruct((2 * ROW, ROW), f32),
        in_specs=[vmem] * 3,
        out_specs=vmem,
        compiler_params=pltpu.CompilerParams(vmem_limit_bytes=4 << 20),
        name="integrals",
    )(local, both, rest)
    perturbed = y.reshape(levels, ROW, 4, ROW).transpose(2, 0, 1, 3).reshape(tendencies.shape)
    integrals = out.reshape(ROW, 2, ROW).transpose(1, 0, 2).reshape(2, ROW * ROW)
    return perturbed, integrals


def solution(mesh):
    split = jax.sharding.Mesh(mesh.devices.reshape(4, 4, 4, 4), ("x", "z", "y", "lev"))
    band = ("x", "z", "y")
    in_specs = (P(band, None), P("lev"), P("lev"), P(band), P(None, "lev", band))
    out_specs = (P(None, "lev", band), P(None, band))
    return jax.shard_map(program, mesh=split, in_specs=in_specs, out_specs=out_specs, check_vma=False)
```

```python
import jax
import jax.numpy as jnp
from jax import lax
from jax.experimental import pallas as pl
from jax.experimental.pallas import tpu as pltpu
from jax.sharding import PartitionSpec as P


OFFSET = (0, 3, 1, 2)
SOURCE = (0, 2, 1, 3)
ROW = 128
LEVELS = 40
PARTS = 8
PART = 4 * ROW // PARTS
HEAD = 22


def along_z(a):
    pairs = []
    for z in range(4):
        for lev in range(4):
            pairs.append((((z + OFFSET[lev]) % 4) * 4 + SOURCE[lev], z * 4 + lev))
    return lax.ppermute(a, ("z", "lev"), pairs)


def along_y(a, step):
    return lax.ppermute(a, "y", [(y, (y + step) % 4) for y in range(4)])


def along_x(a, step):
    return lax.ppermute(a, "x", [(x, (x + step) % 4) for x in range(4)])


def across_lev(a, flip):
    return lax.ppermute(a, "lev", [(i, i ^ flip) for i in range(4)])


def iota(shape, dim):
    return lax.broadcasted_iota(jnp.int32, shape, dim)


def onehot(cond):
    return jnp.where(cond, 1.0, 0.0).astype(jnp.bfloat16)


def dot(a, b):
    return jnp.dot(a, b, preferred_element_type=jnp.float32)


def dot_nt(a, b):
    return lax.dot_general(a, b, (((1,), (1,)), ((), ())), preferred_element_type=jnp.float32)


def three_parts(v):
    high = v.astype(jnp.bfloat16)
    rest = v - high.astype(jnp.float32)
    mid = rest.astype(jnp.bfloat16)
    low = (rest - mid.astype(jnp.float32)).astype(jnp.bfloat16)
    return high, mid, low


def parts_of(source):
    band, row = source >> 7, source & 127
    offset = ((band >> 2) - lax.axis_index("z")) & 3
    lev = jnp.where(offset == 3, 1, jnp.where(offset == 0, 0, offset + 1))
    return band >> 4, lev, (lax.axis_index("y") - band) & 3, row


def prepare_kernel(source_ref, taper_ref, thick_ref, scalars_ref):
    source = source_ref[...]
    x, lev, table, _ = parts_of(source)
    holder = (x * 4 + lev) * 4 + table
    member = iota((64, ROW), 0) == holder
    before = onehot(iota((ROW, ROW), 0) < iota((ROW, ROW), 1))
    count = dot(onehot(member), before)
    rank = jnp.sum(jnp.where(member, count, 0.0), axis=0, keepdims=True)
    pos = holder * 2 + rank.astype(jnp.int32)

    taper, thick = taper_ref[...], thick_ref[...]
    levels = taper.shape[1]
    diagonal = iota((LEVELS, levels), 0) == iota((LEVELS, levels), 1)

    def one_per_row(v):
        total = jnp.sum(jnp.where(diagonal, jnp.broadcast_to(v, diagonal.shape), 0.0), axis=1, keepdims=True)
        return jnp.broadcast_to(total, (LEVELS, ROW))

    scalars_ref[0:LEVELS, :] = one_per_row(taper)
    scalars_ref[LEVELS : 2 * LEVELS, :] = one_per_row(taper * thick)
    scalars_ref[2 * LEVELS : 2 * LEVELS + 8, :] = jnp.broadcast_to(jnp.sum(thick * thick, axis=1, keepdims=True), (8, ROW))
    scalars_ref[2 * LEVELS + 8 : 2 * LEVELS + 16, :] = jnp.broadcast_to(pos.astype(jnp.float32), (8, ROW))
    scalars_ref[2 * LEVELS + 16 :, :] = jnp.broadcast_to(source.astype(jnp.float32), (8, ROW))


def wanted_kernel(scalars_ref, from1, from2, from3, ids_ref):
    slot = iota((ROW, ROW), 0)
    step = (lax.axis_index("x") - (slot >> 5)) & 3
    own = scalars_ref[2 * LEVELS + 16 : 2 * LEVELS + 17, :].astype(jnp.int32)
    source = jnp.where(step == 0, own, jnp.where(step == 1, from1[...], jnp.where(step == 2, from2[...], from3[...])))
    x, lev, table, row = parts_of(source)
    mine = (x == lax.axis_index("x")) & (lev == lax.axis_index("lev")) & (table == ((slot >> 1) & 3))
    before = onehot(iota((ROW, ROW), 0) < iota((ROW, ROW), 1))
    count = dot(onehot(mine), before)
    chosen = mine & (count == (slot & 1).astype(jnp.float32))
    ids = jnp.sum(jnp.where(chosen, (table * ROW + row).astype(jnp.float32), 0.0), axis=1, keepdims=True)
    ids_ref[...] = jnp.broadcast_to(ids, (ROW, ROW)).astype(jnp.int32)


def pick_kernel(ids_ref, t0, t1, t2, t3, out_ref):
    ids, lane = ids_ref[...], iota((ROW, ROW), 1)
    total = None
    for c, ref in enumerate((t0, t1, t2, t3)):
        pick = onehot(ids == lane + c * ROW)
        part = tuple(dot(pick, v) for v in three_parts(ref[...]))
        total = part if total is None else tuple(a + b for a, b in zip(total, part))
    out_ref[...] = (total[0] + total[1]) + total[2]


def fetches(pieces):
    def copies(i):
        rows = pl.ds(pl.multiple_of(i * PART, PART), PART)
        return [pltpu.make_async_copy(a.at[:, rows, :], b.at[:, rows, :], sems.at[i]) for a, b, sems in pieces]

    for i in range(PARTS):
        for copy in copies(i):
            copy.start()

    def wait(i):
        for copy in copies(i):
            copy.wait()

    return wait


def column_kernel(scalars_ref, x_hbm, sums_ref, place_ref, head_ref, acc_ref, tail_ref, head_sems, sems):
    levels = x_hbm.shape[0]
    wait = fetches([(x_hbm.at[:HEAD], head_ref, head_sems), (x_hbm.at[HEAD:], tail_ref, sems)])
    pos = jnp.broadcast_to(scalars_ref[2 * LEVELS + 8 : 2 * LEVELS + 9, :], (ROW, ROW)).astype(jnp.bfloat16)
    expand = onehot(iota((4 * ROW, ROW), 0) >> 2 == iota((4 * ROW, ROW), 1))
    slot = dot_nt(expand, pos).astype(jnp.int32)
    place_ref[...] = onehot(slot == iota((4 * ROW, ROW), 1))

    def chunk(i, carry):
        wait(i)
        for r in range(0, PART, 64):
            rows = pl.ds(pl.multiple_of(i * PART + r, 64), 64)
            acc = head_ref[0, rows, :].astype(jnp.float32) * scalars_ref[LEVELS : LEVELS + 1, :]
            for l in range(1, levels):
                here = head_ref[l, rows, :] if l < HEAD else tail_ref[l - HEAD, rows, :]
                acc = acc + here.astype(jnp.float32) * scalars_ref[LEVELS + l : LEVELS + l + 1, :]
            acc_ref[rows, :] = acc
        return carry

    lax.fori_loop(0, PARTS, chunk, 0)
    for k in range(2):
        sums_ref[pl.ds(k * ROW, ROW), :] = acc_ref[pl.ds(2 + k, ROW, stride=4), :]
    sums_ref[pl.ds(2 * ROW, 8), :] = scalars_ref[2 * LEVELS : 2 * LEVELS + 8, :]


def perturb_kernel(scalars_ref, arrived_ref, place_ref, head_ref, x_hbm, y_hbm, clipped_ref, local_ref, x_ref, y_ref, in_sems, sems):
    levels = y_ref.shape[0]
    wait = fetches([(x_hbm.at[HEAD:], x_ref, in_sems)])
    parts = three_parts(jnp.tanh(arrived_ref[...]))
    place = place_ref[...]
    local_ref[...] = (dot(place, parts[0]) + dot(place, parts[1])) + dot(place, parts[2])

    def store(i):
        rows = pl.ds(pl.multiple_of(i * PART, PART), PART)
        return pltpu.make_async_copy(y_ref.at[:, rows, :], y_hbm.at[:, rows, :], sems.at[i])

    def chunk(i, carry):
        wait(i)
        for r in range(0, PART, 32):
            rows = pl.ds(pl.multiple_of(i * PART + r, 32), 32)
            local = local_ref[rows, :]
            for l in range(levels):
                scale = 1.0 + scalars_ref[l : l + 1, :] * local
                here = head_ref[l, rows, :] if l < HEAD else x_ref[l - HEAD, rows, :]
                y_ref[l, rows, :] = (here.astype(jnp.float32) * scale).astype(jnp.bfloat16)
        store(i).start()
        return carry

    lax.fori_loop(0, PARTS, chunk, 0)

    clipped_ref[...] = local_ref[pl.ds(0, ROW, stride=4), :]
    for i in range(PARTS):
        store(i).wait()


def add_kernel(a_ref, b_ref, out_ref):
    out_ref[...] = a_ref[...] + b_ref[...]


def integrals_kernel(local_ref, s0, s1, out_ref):
    local = local_ref[...]
    total = s0[...] + s1[...]
    norm = jnp.sqrt(total[2 * ROW : 2 * ROW + 1, :])
    for k in range(2):
        out_ref[pl.ds(k, ROW, stride=2), :] = local * total[k * ROW : (k + 1) * ROW, :] / norm


def program(pattern, taper, thickness, block_source, tendencies):
    vmem, hbm = pl.BlockSpec(memory_space=pltpu.VMEM), pl.BlockSpec(memory_space=pltpu.HBM)
    levels = tendencies.shape[1]
    f32, s32 = jnp.float32, jnp.int32

    table = along_z(pattern)
    source = block_source.reshape(1, ROW)
    asked = [along_x(source, k) for k in (1, 2, 3)]
    scalars = pl.pallas_call(
        prepare_kernel,
        out_shape=jax.ShapeDtypeStruct((2 * LEVELS + 24, ROW), f32),
        in_specs=[vmem] * 3,
        out_specs=vmem,
        name="prepare",
    )(source, taper.reshape(1, levels), thickness.reshape(1, levels))
    tables = [table] + [along_y(table, k) for k in (1, 2, 3)]
    wanted = pl.pallas_call(
        wanted_kernel,
        out_shape=jax.ShapeDtypeStruct((ROW, ROW), s32),
        in_specs=[vmem] * 4,
        out_specs=vmem,
        compiler_params=pltpu.CompilerParams(vmem_limit_bytes=4 << 20),
        name="wanted",
    )(scalars, *asked)

    x = tendencies.reshape(4, levels, ROW, ROW).transpose(1, 2, 0, 3).reshape(levels, 4 * ROW, ROW)
    sums, place, head = pl.pallas_call(
        column_kernel,
        out_shape=(
            jax.ShapeDtypeStruct((2 * ROW + 8, ROW), f32),
            jax.ShapeDtypeStruct((4 * ROW, ROW), jnp.bfloat16),
            jax.ShapeDtypeStruct((HEAD, 4 * ROW, ROW), x.dtype),
        ),
        in_specs=[vmem, hbm],
        out_specs=(vmem, vmem, vmem),
        scratch_shapes=[
            pltpu.VMEM((4 * ROW, ROW), f32),
            pltpu.VMEM((levels - HEAD, 4 * ROW, ROW), x.dtype),
            pltpu.SemaphoreType.DMA((PARTS,)),
            pltpu.SemaphoreType.DMA((PARTS,)),
        ],
        cost_estimate=pl.CostEstimate(flops=10_000_000, bytes_accessed=4_500_000, transcendentals=0),
        compiler_params=pltpu.CompilerParams(vmem_limit_bytes=50 << 20),
        name="columns",
    )(scalars, x)
    pair = across_lev(sums, 1)
    both = pl.pallas_call(
        add_kernel,
        out_shape=jax.ShapeDtypeStruct(sums.shape, f32),
        in_specs=[vmem] * 2,
        out_specs=vmem,
        compiler_params=pltpu.CompilerParams(vmem_limit_bytes=4 << 20),
        name="both",
    )(sums, pair)
    rest = across_lev(both, 2)

    picked = pl.pallas_call(
        pick_kernel,
        out_shape=jax.ShapeDtypeStruct((ROW, ROW), f32),
        in_specs=[vmem] * 5,
        out_specs=vmem,
        compiler_params=pltpu.CompilerParams(vmem_limit_bytes=4 << 20),
        name="pick",
    )(wanted, *tables)
    arrived = lax.all_to_all(picked.reshape(16, 8, ROW), ("x", "lev"), 0, 0, tiled=True).reshape(ROW, ROW)

    y, local = pl.pallas_call(
        perturb_kernel,
        out_shape=(jax.ShapeDtypeStruct(x.shape, x.dtype), jax.ShapeDtypeStruct((ROW, ROW), f32)),
        in_specs=[vmem, vmem, vmem, vmem, hbm],
        out_specs=(hbm, vmem),
        scratch_shapes=[
            pltpu.VMEM((4 * ROW, ROW), f32),
            pltpu.VMEM((levels - HEAD, 4 * ROW, ROW), x.dtype),
            pltpu.VMEM(x.shape, x.dtype),
            pltpu.SemaphoreType.DMA((PARTS,)),
            pltpu.SemaphoreType.DMA((PARTS,)),
        ],
        cost_estimate=pl.CostEstimate(flops=10_000_000, bytes_accessed=9_000_000, transcendentals=0),
        compiler_params=pltpu.CompilerParams(vmem_limit_bytes=50 << 20),
        name="perturb",
    )(scalars, arrived, place, head, x)
    out = pl.pallas_call(
        integrals_kernel,
        out_shape=jax.ShapeDtypeStruct((2 * ROW, ROW), f32),
        in_specs=[vmem] * 3,
        out_specs=vmem,
        compiler_params=pltpu.CompilerParams(vmem_limit_bytes=4 << 20),
        name="integrals",
    )(local, both, rest)
    perturbed = y.reshape(levels, ROW, 4, ROW).transpose(2, 0, 1, 3).reshape(tendencies.shape)
    integrals = out.reshape(ROW, 2, ROW).transpose(1, 0, 2).reshape(2, ROW * ROW)
    return perturbed, integrals


def solution(mesh):
    split = jax.sharding.Mesh(mesh.devices.reshape(4, 4, 4, 4), ("x", "z", "y", "lev"))
    band = ("x", "z", "y")
    in_specs = (P(band, None), P("lev"), P("lev"), P(band), P(None, "lev", band))
    out_specs = (P(None, "lev", band), P(None, band))
    return jax.shard_map(program, mesh=split, in_specs=in_specs, out_specs=out_specs, check_vma=False)
```

```python
import jax
import jax.numpy as jnp
from jax import lax
from jax.experimental import pallas as pl
from jax.experimental.pallas import tpu as pltpu
from jax.sharding import PartitionSpec as P


OFFSET = (0, 3, 1, 2)
SOURCE = (0, 2, 1, 3)
ROW = 128
LEVELS = 40
PARTS = 8
PART = 4 * ROW // PARTS
HEAD = 22


def along_z(a):
    pairs = []
    for z in range(4):
        for lev in range(4):
            pairs.append((((z + OFFSET[lev]) % 4) * 4 + SOURCE[lev], z * 4 + lev))
    return lax.ppermute(a, ("z", "lev"), pairs)


def along_y(a, step):
    return lax.ppermute(a, "y", [(y, (y + step) % 4) for y in range(4)])


def along_x(a, step):
    return lax.ppermute(a, "x", [(x, (x + step) % 4) for x in range(4)])


def across_lev(a, flip):
    return lax.ppermute(a, "lev", [(i, i ^ flip) for i in range(4)])


def iota(shape, dim):
    return lax.broadcasted_iota(jnp.int32, shape, dim)


def onehot(cond):
    return jnp.where(cond, 1.0, 0.0).astype(jnp.bfloat16)


def dot(a, b):
    return jnp.dot(a, b, preferred_element_type=jnp.float32)


def dot_nt(a, b):
    return lax.dot_general(a, b, (((1,), (1,)), ((), ())), preferred_element_type=jnp.float32)


def three_parts(v):
    high = v.astype(jnp.bfloat16)
    rest = v - high.astype(jnp.float32)
    mid = rest.astype(jnp.bfloat16)
    low = (rest - mid.astype(jnp.float32)).astype(jnp.bfloat16)
    return high, mid, low


def parts_of(source):
    band, row = source >> 7, source & 127
    offset = ((band >> 2) - lax.axis_index("z")) & 3
    lev = jnp.where(offset == 3, 1, jnp.where(offset == 0, 0, offset + 1))
    return band >> 4, lev, (lax.axis_index("y") - band) & 3, row


def prepare_kernel(packed_ref, scalars_ref):
    source = packed_ref[0:1, :].astype(jnp.int32)
    x, lev, table, _ = parts_of(source)
    holder = (x * 4 + lev) * 4 + table
    member = iota((64, ROW), 0) == holder
    before = onehot(iota((ROW, ROW), 0) < iota((ROW, ROW), 1))
    count = dot(onehot(member), before)
    rank = jnp.sum(jnp.where(member, count, 0.0), axis=0, keepdims=True)
    pos = holder * 2 + rank.astype(jnp.int32)

    taper, thick = packed_ref[1:2, :], packed_ref[2:3, :]
    levels = taper.shape[1]
    diagonal = iota((LEVELS, levels), 0) == iota((LEVELS, levels), 1)

    def one_per_row(v):
        total = jnp.sum(jnp.where(diagonal, jnp.broadcast_to(v, diagonal.shape), 0.0), axis=1, keepdims=True)
        return jnp.broadcast_to(total, (LEVELS, ROW))

    scalars_ref[0:LEVELS, :] = one_per_row(taper)
    scalars_ref[LEVELS : 2 * LEVELS, :] = one_per_row(taper * thick)
    scalars_ref[2 * LEVELS : 2 * LEVELS + 8, :] = jnp.broadcast_to(jnp.sum(thick * thick, axis=1, keepdims=True), (8, ROW))
    scalars_ref[2 * LEVELS + 8 : 2 * LEVELS + 16, :] = jnp.broadcast_to(pos.astype(jnp.float32), (8, ROW))
    scalars_ref[2 * LEVELS + 16 :, :] = jnp.broadcast_to(source.astype(jnp.float32), (8, ROW))


def wanted_kernel(scalars_ref, from1, from2, from3, ids_ref):
    slot = iota((ROW, ROW), 0)
    step = (lax.axis_index("x") - (slot >> 5)) & 3
    own = scalars_ref[2 * LEVELS + 16 : 2 * LEVELS + 17, :].astype(jnp.int32)
    source = jnp.where(step == 0, own, jnp.where(step == 1, from1[...], jnp.where(step == 2, from2[...], from3[...])))
    x, lev, table, row = parts_of(source)
    mine = (x == lax.axis_index("x")) & (lev == lax.axis_index("lev")) & (table == ((slot >> 1) & 3))
    before = onehot(iota((ROW, ROW), 0) < iota((ROW, ROW), 1))
    count = dot(onehot(mine), before)
    chosen = mine & (count == (slot & 1).astype(jnp.float32))
    ids = jnp.sum(jnp.where(chosen, (table * ROW + row).astype(jnp.float32), 0.0), axis=1, keepdims=True)
    ids_ref[...] = jnp.broadcast_to(ids, (ROW, ROW)).astype(jnp.int32)


def pick_kernel(ids_ref, t0, t1, t2, t3, out_ref):
    ids, lane = ids_ref[...], iota((ROW, ROW), 1)
    total = None
    for c, ref in enumerate((t0, t1, t2, t3)):
        pick = onehot(ids == lane + c * ROW)
        part = tuple(dot(pick, v) for v in three_parts(ref[...]))
        total = part if total is None else tuple(a + b for a, b in zip(total, part))
    out_ref[...] = (total[0] + total[1]) + total[2]


def fetches(pieces):
    def copies(i):
        rows = pl.ds(pl.multiple_of(i * PART, PART), PART)
        return [pltpu.make_async_copy(a.at[:, rows, :], b.at[:, rows, :], sems.at[i]) for a, b, sems in pieces]

    for i in range(PARTS):
        for copy in copies(i):
            copy.start()

    def wait(i):
        for copy in copies(i):
            copy.wait()

    return wait


def column_kernel(scalars_ref, x_hbm, sums_ref, place_ref, head_ref, acc_ref, tail_ref, head_sems, sems):
    levels = x_hbm.shape[0]
    wait = fetches([(x_hbm.at[:HEAD], head_ref, head_sems), (x_hbm.at[HEAD:], tail_ref, sems)])
    pos = jnp.broadcast_to(scalars_ref[2 * LEVELS + 8 : 2 * LEVELS + 9, :], (ROW, ROW)).astype(jnp.bfloat16)
    expand = onehot(iota((4 * ROW, ROW), 0) >> 2 == iota((4 * ROW, ROW), 1))
    slot = dot_nt(expand, pos).astype(jnp.int32)
    place_ref[...] = onehot(slot == iota((4 * ROW, ROW), 1))

    def chunk(i, carry):
        wait(i)
        for r in range(0, PART, 64):
            rows = pl.ds(pl.multiple_of(i * PART + r, 64), 64)
            acc = head_ref[0, rows, :].astype(jnp.float32) * scalars_ref[LEVELS : LEVELS + 1, :]
            for l in range(1, levels):
                here = head_ref[l, rows, :] if l < HEAD else tail_ref[l - HEAD, rows, :]
                acc = acc + here.astype(jnp.float32) * scalars_ref[LEVELS + l : LEVELS + l + 1, :]
            acc_ref[rows, :] = acc
        return carry

    lax.fori_loop(0, PARTS, chunk, 0)
    for k in range(2):
        sums_ref[pl.ds(k * ROW, ROW), :] = acc_ref[pl.ds(2 + k, ROW, stride=4), :]
    sums_ref[pl.ds(2 * ROW, 8), :] = scalars_ref[2 * LEVELS : 2 * LEVELS + 8, :]


def perturb_kernel(scalars_ref, arrived_ref, place_ref, head_ref, x_hbm, y_hbm, clipped_ref, local_ref, x_ref, y_ref, in_sems, sems):
    levels = y_ref.shape[0]
    wait = fetches([(x_hbm.at[HEAD:], x_ref, in_sems)])
    parts = three_parts(jnp.tanh(arrived_ref[...]))
    place = place_ref[...]
    local_ref[...] = (dot(place, parts[0]) + dot(place, parts[1])) + dot(place, parts[2])

    def store(i):
        rows = pl.ds(pl.multiple_of(i * PART, PART), PART)
        return pltpu.make_async_copy(y_ref.at[:, rows, :], y_hbm.at[:, rows, :], sems.at[i])

    def chunk(i, carry):
        wait(i)
        for r in range(0, PART, 32):
            rows = pl.ds(pl.multiple_of(i * PART + r, 32), 32)
            local = local_ref[rows, :]
            for l in range(levels):
                scale = 1.0 + scalars_ref[l : l + 1, :] * local
                here = head_ref[l, rows, :] if l < HEAD else x_ref[l - HEAD, rows, :]
                y_ref[l, rows, :] = (here.astype(jnp.float32) * scale).astype(jnp.bfloat16)
        store(i).start()
        return carry

    lax.fori_loop(0, PARTS, chunk, 0)

    clipped_ref[...] = local_ref[pl.ds(0, ROW, stride=4), :]
    for i in range(PARTS):
        store(i).wait()


def add_kernel(a_ref, b_ref, out_ref):
    out_ref[...] = a_ref[...] + b_ref[...]


def integrals_kernel(local_ref, s0, s1, out_ref):
    local = local_ref[...]
    total = s0[...] + s1[...]
    norm = jnp.sqrt(total[2 * ROW : 2 * ROW + 1, :])
    for k in range(2):
        out_ref[pl.ds(k, ROW, stride=2), :] = local * total[k * ROW : (k + 1) * ROW, :] / norm


def program(pattern, taper, thickness, block_source, tendencies):
    vmem, hbm = pl.BlockSpec(memory_space=pltpu.VMEM), pl.BlockSpec(memory_space=pltpu.HBM)
    levels = tendencies.shape[1]
    f32, s32 = jnp.float32, jnp.int32

    table = along_z(pattern)
    source = block_source.reshape(1, ROW)
    asked = [along_x(source, k) for k in (1, 2, 3)]
    room = (0, ROW - levels)
    packed = jnp.stack([block_source.astype(f32), jnp.pad(taper, room), jnp.pad(thickness, room)])
    scalars = pl.pallas_call(
        prepare_kernel,
        out_shape=jax.ShapeDtypeStruct((2 * LEVELS + 24, ROW), f32),
        in_specs=[vmem],
        out_specs=vmem,
        compiler_params=pltpu.CompilerParams(vmem_limit_bytes=4 << 20),
        name="prepare",
    )(packed)
    tables = [table] + [along_y(table, k) for k in (1, 2, 3)]
    wanted = pl.pallas_call(
        wanted_kernel,
        out_shape=jax.ShapeDtypeStruct((ROW, ROW), s32),
        in_specs=[vmem] * 4,
        out_specs=vmem,
        compiler_params=pltpu.CompilerParams(vmem_limit_bytes=4 << 20),
        name="wanted",
    )(scalars, *asked)

    x = tendencies.reshape(4, levels, ROW, ROW).transpose(1, 2, 0, 3).reshape(levels, 4 * ROW, ROW)
    sums, place, head = pl.pallas_call(
        column_kernel,
        out_shape=(
            jax.ShapeDtypeStruct((2 * ROW + 8, ROW), f32),
            jax.ShapeDtypeStruct((4 * ROW, ROW), jnp.bfloat16),
            jax.ShapeDtypeStruct((HEAD, 4 * ROW, ROW), x.dtype),
        ),
        in_specs=[vmem, hbm],
        out_specs=(vmem, vmem, vmem),
        scratch_shapes=[
            pltpu.VMEM((4 * ROW, ROW), f32),
            pltpu.VMEM((levels - HEAD, 4 * ROW, ROW), x.dtype),
            pltpu.SemaphoreType.DMA((PARTS,)),
            pltpu.SemaphoreType.DMA((PARTS,)),
        ],
        cost_estimate=pl.CostEstimate(flops=10_000_000, bytes_accessed=4_500_000, transcendentals=0),
        compiler_params=pltpu.CompilerParams(vmem_limit_bytes=50 << 20),
        name="columns",
    )(scalars, x)
    pair = across_lev(sums, 1)
    both = pl.pallas_call(
        add_kernel,
        out_shape=jax.ShapeDtypeStruct(sums.shape, f32),
        in_specs=[vmem] * 2,
        out_specs=vmem,
        compiler_params=pltpu.CompilerParams(vmem_limit_bytes=4 << 20),
        name="both",
    )(sums, pair)
    rest = across_lev(both, 2)

    picked = pl.pallas_call(
        pick_kernel,
        out_shape=jax.ShapeDtypeStruct((ROW, ROW), f32),
        in_specs=[vmem] * 5,
        out_specs=vmem,
        compiler_params=pltpu.CompilerParams(vmem_limit_bytes=4 << 20),
        name="pick",
    )(wanted, *tables)
    arrived = lax.all_to_all(picked.reshape(16, 8, ROW), ("x", "lev"), 0, 0, tiled=True).reshape(ROW, ROW)

    y, local = pl.pallas_call(
        perturb_kernel,
        out_shape=(jax.ShapeDtypeStruct(x.shape, x.dtype), jax.ShapeDtypeStruct((ROW, ROW), f32)),
        in_specs=[vmem, vmem, vmem, vmem, hbm],
        out_specs=(hbm, vmem),
        scratch_shapes=[
            pltpu.VMEM((4 * ROW, ROW), f32),
            pltpu.VMEM((levels - HEAD, 4 * ROW, ROW), x.dtype),
            pltpu.VMEM(x.shape, x.dtype),
            pltpu.SemaphoreType.DMA((PARTS,)),
            pltpu.SemaphoreType.DMA((PARTS,)),
        ],
        cost_estimate=pl.CostEstimate(flops=10_000_000, bytes_accessed=9_000_000, transcendentals=0),
        compiler_params=pltpu.CompilerParams(vmem_limit_bytes=50 << 20),
        name="perturb",
    )(scalars, arrived, place, head, x)
    out = pl.pallas_call(
        integrals_kernel,
        out_shape=jax.ShapeDtypeStruct((2 * ROW, ROW), f32),
        in_specs=[vmem] * 3,
        out_specs=vmem,
        compiler_params=pltpu.CompilerParams(vmem_limit_bytes=4 << 20),
        name="integrals",
    )(local, both, rest)
    perturbed = y.reshape(levels, ROW, 4, ROW).transpose(2, 0, 1, 3).reshape(tendencies.shape)
    integrals = out.reshape(ROW, 2, ROW).transpose(1, 0, 2).reshape(2, ROW * ROW)
    return perturbed, integrals


def solution(mesh):
    split = jax.sharding.Mesh(mesh.devices.reshape(4, 4, 4, 4), ("x", "z", "y", "lev"))
    band = ("x", "z", "y")
    in_specs = (P(band, None), P("lev"), P("lev"), P(band), P(None, "lev", band))
    out_specs = (P(None, "lev", band), P(None, band))
    return jax.shard_map(program, mesh=split, in_specs=in_specs, out_specs=out_specs, check_vma=False)
```
